256 devices in a mesh: ep: 16 (over y, x), fsdp: 16 (over z, core).
Axes of the slice: x: 4, y: 4, z: 8, core: 2. Of those that a mesh axis runs over, the one named last changes fastest.
Arguments:
- w_gate: float32 [64, 2048, 1024], P('ep', 'fsdp'), may hold values from -0.1875 to 0.1875
- avg_gate: bfloat16 [64, 2048, 1024], P('ep', 'fsdp'), may hold values from -0.0625 to 0.0625
- w_up: float32 [64, 2048, 1024], P('ep', 'fsdp'), may hold values from -0.1875 to 0.1875
- avg_up: bfloat16 [64, 2048, 1024], P('ep', 'fsdp'), may hold values from -0.0625 to 0.0625
- w_down: float32 [64, 1024, 2048], P('ep', None, 'fsdp'), may hold values from -0.25 to 0.25
- avg_down: bfloat16 [64, 1024, 2048], P('ep', None, 'fsdp'), may hold values from -0.09375 to 0.09375
- router_weight: float32 [2048, 64], P('fsdp', 'ep'), may hold values from -0.125 to 0.125
- router_gain: float32 [2048], P('fsdp'), may hold values from 0.25 to 1.75
Outputs:
- serve_gate: bfloat16 [64, 2048, 1024], P('ep', None, 'fsdp')
- serve_up: bfloat16 [64, 2048, 1024], P('ep', None, 'fsdp')
- serve_down: bfloat16 [64, 1024, 2048], P('ep', 'fsdp')
- scale_gate: float32 [64, 1024], P('ep', 'fsdp')
- scale_up: float32 [64, 1024], P('ep', 'fsdp')
- scale_down: float32 [64, 1024], P('ep', 'fsdp')
- serve_router: bfloat16 [2048, 64], replicated
The draws below stay inside these ranges and needn't reach their ends.
All inputs are finite; a program needn't handle non-finite values.
Results may differ from the reference program's by a relative error of at most 0.001.
Values may be sent and summed in bfloat16 or wider, within the bound.
No kernel may reach another device: no remote copies, remote signals or barrier semaphores. Data moves between devices by JAX's collectives and lax.ppermute only.
A program may use at most 64 MiB of HBM per device.

```python
import jax
import jax.numpy as jnp
from jax import lax

EXPERTS = 64
D_MODEL = 2048
D_EXPERT = 1024


def with_spikes(result, stream_key, source, target, blocks, factor):
    owner, partner = [(jnp.arange(result.shape[axis_at]) // (result.shape[axis_at] // blocks)).reshape([-1 if axis == axis_at else 1 for axis in range(result.ndim)]) for axis_at in (source, target)]
    chosen = jax.random.permutation(stream_key, blocks)[partner]
    strong = (owner == chosen) | (owner == (partner + blocks // 2) % blocks)
    return jnp.where(strong, factor * result, result)


def levels(rng, shape, split, least, top_value):
    gain, own = 1.0, jax.random.fold_in(rng, 6)
    for position, shards_of in split:
        steps = jnp.exp(jax.random.uniform(jax.random.fold_in(own, position), (shards_of,), jnp.float32, least / len(split), top_value / len(split)))
        gain = gain * jnp.repeat(steps, shape[position] // shards_of).reshape([-1 if axis == position else 1 for axis in range(len(shape))])
    return gain


def centred(rng, dims, width, bound, cuts=(), kind=jnp.bfloat16):
    drawn = jax.random.normal(rng, dims, jnp.float32) * width
    if len(cuts) > 0:
        drawn = levels(rng, dims, cuts, -0.22, 0.18) * drawn
    return jnp.clip(drawn, min=-bound, max=bound).astype(kind)


def gaussian_with(stream_key, shape, spread, reach, split, heavy, dtype=jnp.bfloat16):
    values = spread * jax.random.normal(stream_key, shape, jnp.float32)
    if split:
        values = values * levels(stream_key, shape, split, -0.22, 0.18)
    return jnp.clip(with_spikes(values, jax.random.fold_in(stream_key, 3), *heavy), -reach, reach).astype(dtype)


def setup_inputs(seed: int = 0) -> dict:
    splits = jax.random.split(jax.random.key(seed), 9)
    w_gate = gaussian_with(splits[0], (EXPERTS, D_MODEL, D_EXPERT), D_MODEL ** -0.5, 0.1875, ((0, 16), (1, 16)), (1, 2, 16, 2.0), jnp.float32)
    avg_gate = centred(splits[1], (EXPERTS, D_MODEL, D_EXPERT), (D_MODEL * 4) ** -0.5, 0.0625, ((0, 16), (1, 16)))
    w_up = gaussian_with(splits[2], (EXPERTS, D_MODEL, D_EXPERT), D_MODEL ** -0.5, 0.1875, ((0, 16), (1, 16)), (1, 2, 16, 2.0), jnp.float32)
    avg_up = centred(splits[3], (EXPERTS, D_MODEL, D_EXPERT), (D_MODEL * 4) ** -0.5, 0.0625, ((0, 16), (1, 16)))
    w_down = gaussian_with(splits[4], (EXPERTS, D_EXPERT, D_MODEL), D_EXPERT ** -0.5, 0.25, ((0, 16), (2, 16)), (2, 1, 16, 2.0), jnp.float32)
    avg_down = centred(splits[5], (EXPERTS, D_EXPERT, D_MODEL), (D_EXPERT * 4) ** -0.5, 0.09375, ((0, 16), (2, 16)))
    router_weight = centred(splits[6], (D_MODEL, EXPERTS), D_MODEL ** -0.5, 0.125, ((0, 16), (1, 16)), jnp.float32)
    router_gain = jnp.clip(1.0 + 0.15 * jax.random.normal(splits[7], (D_MODEL,), jnp.float32), 0.25, 1.75)
    return {"w_gate": w_gate, "avg_gate": avg_gate, "w_up": w_up, "avg_up": avg_up, "w_down": w_down, "avg_down": avg_down, "router_weight": router_weight, "router_gain": router_gain}


def reference(w_gate, avg_gate, w_up, avg_up, w_down, avg_down, router_weight, router_gain):
    fresh_gate = w_gate + avg_gate.astype(jnp.float32)
    fresh_up = w_up + avg_up.astype(jnp.float32)
    fresh_down = w_down + avg_down.astype(jnp.float32)
    scale_gate = jnp.sqrt(lax.optimization_barrier(jnp.sum(fresh_gate * fresh_gate, axis=1)))
    serve_gate = (fresh_gate / jnp.expand_dims(scale_gate, 1)).astype(jnp.bfloat16)
    scale_up = jnp.sqrt(lax.optimization_barrier(jnp.sum(fresh_up * fresh_up, axis=1)))
    serve_up = (fresh_up / jnp.expand_dims(scale_up, 1)).astype(jnp.bfloat16)
    scale_down = jnp.sqrt(lax.optimization_barrier(jnp.sum(fresh_down * fresh_down, axis=2)))
    serve_down = (fresh_down / jnp.expand_dims(scale_down, 2)).astype(jnp.bfloat16)
    serve_router = (router_weight * router_gain[:, None]).astype(jnp.bfloat16)
    return (serve_gate, serve_up, serve_down, scale_gate, scale_up, scale_down, serve_router)
```

```python
import jax
import jax.numpy as jnp
from jax import lax
from jax.experimental import pallas as pl
from jax.experimental.pallas import tpu as pltpu
from jax.sharding import PartitionSpec as P


CHIPS = 8
POWER = 17.0
LIFT = 2.0 ** (126.0 / 17.0)
TINY = 1e-37

PARTNERS = (
    (3, 0), (5, 0), (2, 0), (6, 0), (4, 0), (4, 1), (3, 1), (5, 1),
    (2, 1), (6, 1), (1, 0), (7, 0), (1, 1), (7, 1), (0, 1),
)


def encode_kernel(
    wg, ag, wu, au, wd, ad, router, gain, *refs
):
    pieces, slab_ref = refs[:16], refs[16]
    buf_g, buf_ag, buf_u, buf_au, buf_d, buf_ad, out_buf, rows, in_sem, out_sem = refs[17:]
    me = lax.axis_index("fsdp")
    chip, core = lax.shift_right_logical(me, 1), lax.bitwise_and(me, 1)

    def columns(g):
        return pl.ds(pl.multiple_of(lax.rem(chip + g, CHIPS) * 128, 128), 128)

    def fetch(g):
        at = columns(g)
        return [
            pltpu.make_async_copy(wg.at[:, :, at], buf_g.at[g], in_sem.at[g, 0]),
            pltpu.make_async_copy(ag.at[:, :, at], buf_ag.at[g], in_sem.at[g, 1]),
            pltpu.make_async_copy(wu.at[:, :, at], buf_u.at[g], in_sem.at[g, 2]),
            pltpu.make_async_copy(au.at[:, :, at], buf_au.at[g], in_sem.at[g, 3]),
            pltpu.make_async_copy(wd.at[:, at, :], buf_d.at[g], in_sem.at[g, 4]),
            pltpu.make_async_copy(ad.at[:, at, :], buf_ad.at[g], in_sem.at[g, 5]),
        ]

    copies = [fetch(g) for g in range(CHIPS)]
    for group in copies:
        for c in group:
            c.start()
    lane = lax.broadcasted_iota(jnp.int32, (128, 128), 1)
    left = lax.broadcasted_iota(jnp.int32, (6, 128), 1) < 64
    rows[12:16, :] = router[...] * gain[...]

    def power(x):
        x2 = x * x
        x4 = x2 * x2
        x8 = x4 * x4
        return x8 * x8 * x

    stores = []
    for g in range(CHIPS):
        for c in copies[g]:
            c.wait()
        sums = []
        for a, (w, v) in enumerate(((buf_g, buf_ag), (buf_u, buf_au))):
            for e in range(4):
                fresh = w[g, e] + v[g, e].astype(jnp.float32)
                total = jnp.sum(fresh * fresh, axis=0, keepdims=True)
                sums.append(total)
                y = power(fresh * (lax.rsqrt(jnp.maximum(total, TINY)) * LIFT))
                y = y.astype(jnp.bfloat16).T
                q = a * 4 + e
                out_buf[2 * g, q * 64 : q * 64 + 64, :] = y[:64]
                out_buf[2 * g + 1, q * 64 : q * 64 + 64, :] = y[64:]
        tall = jnp.zeros((128, 128), jnp.float32)
        for e in range(4):
            fresh = buf_d[g, e] + buf_ad[g, e].astype(jnp.float32)
            total = jnp.sum(fresh * fresh, axis=1, keepdims=True)
            tall = jnp.where(lane == e, total, tall)
            y = power(fresh * (lax.rsqrt(jnp.maximum(total, TINY)) * LIFT))
            y = y.astype(jnp.bfloat16)
            q = 8 + e
            out_buf[2 * g, q * 64 : q * 64 + 64, :] = y[:64]
            out_buf[2 * g + 1, q * 64 : q * 64 + 64, :] = y[64:]
        for flip in range(2):
            copy = pltpu.make_async_copy(
                out_buf.at[2 * g + lax.bitwise_xor(core, flip)],
                pieces[2 * g + flip],
                out_sem.at[2 * g + flip],
            )
            copy.start()
            stores.append(copy)
        wide = tall.T
        top = jnp.concatenate(sums[:6], axis=0)
        bottom = jnp.concatenate(sums[6:] + [wide[0:4]], axis=0)
        to_first = jnp.where(left, top, pltpu.roll(bottom, 64, 1))
        to_second = jnp.where(left, pltpu.roll(top, 64, 1), bottom)
        to = lax.rem(chip + g, CHIPS) * 2
        for c, s in enumerate((to_first, to_second)):
            high = s.astype(jnp.bfloat16).astype(jnp.float32)
            rows[0:6, :] = high
            rows[6:12, :] = s - high
            slab_ref[to + c] = rows[...].astype(jnp.bfloat16)
    for copy in stores:
        copy.wait()


def encode(arrays, router, gain):
    anywhere = pl.BlockSpec(memory_space=pl.ANY)
    vmem = pl.BlockSpec(memory_space=pltpu.VMEM)
    piece = jax.ShapeDtypeStruct((768, 128), jnp.bfloat16)
    f32, bf16 = jnp.float32, jnp.bfloat16
    return pl.pallas_call(
        encode_kernel,
        in_specs=[anywhere] * 6 + [vmem] * 2,
        out_specs=[anywhere] * 16 + [vmem],
        out_shape=[piece] * 16 + [jax.ShapeDtypeStruct((16, 16, 128), bf16)],
        scratch_shapes=[
            pltpu.VMEM((CHIPS, 4, 128, 128), dtype) for dtype in (f32, bf16) * 3
        ]
        + [
            pltpu.VMEM((16, 768, 128), bf16),
            pltpu.VMEM((16, 128), f32),
            pltpu.SemaphoreType.DMA((CHIPS, 6)),
            pltpu.SemaphoreType.DMA((16,)),
        ],
        cost_estimate=pl.CostEstimate(
            flops=20_000_000, bytes_accessed=12_600_000, transcendentals=0
        ),
        name="encode",
    )(*arrays, router, gain)


def decode_kernel(slab, *refs):
    pieces, outs, scale_ref = refs[:16], refs[16:19], refs[19]
    in_buf, out_buf, factors, in_sem, out_sem = refs[20:]
    me = lax.axis_index("fsdp")
    chip, core = lax.shift_right_logical(me, 1), lax.bitwise_and(me, 1)
    sources = [
        lax.rem(chip + CHIPS - dz, CHIPS) * 2 + lax.bitwise_xor(core, dc)
        for dz, dc in ((0, 0), *PARTNERS)
    ]
    fetches = []
    for k in range(16):
        copy = pltpu.make_async_copy(pieces[k], in_buf.at[k], in_sem.at[k])
        copy.start()
        fetches.append(copy)
    local, total = [], jnp.zeros((6, 128), jnp.float32)
    for k in range(16):
        both = slab[sources[k]].astype(jnp.float32)
        s = both[0:6] + both[6:12]
        local.append(s)
        total = total + s
    scale_ref[...] = jnp.sqrt(total)
    for k in range(16):
        factors[k * 8 : k * 8 + 6, :] = jnp.sqrt(local[k] / total) * (1.0 / LIFT)
        factors[k * 8 + 6 : k * 8 + 8, :] = jnp.zeros((2, 128), jnp.float32)
    across = factors[...].T
    stores = []
    for k in range(16):
        fetches[k].wait()
        for q in range(12):
            half, row = q // 6, q % 6
            factor = across[half * 64 : half * 64 + 64, k * 8 + row : k * 8 + row + 1]
            y = in_buf[k, q * 64 : q * 64 + 64, :].astype(jnp.float32)
            x = jnp.exp2(jnp.log2(jnp.abs(y)) * (1.0 / POWER)) * factor
            out_buf[k, q] = jnp.where(y < 0, -x, x).astype(jnp.bfloat16)
        at = pl.ds(pl.multiple_of(sources[k] * 128, 128), 128)
        for a in range(3):
            copy = pltpu.make_async_copy(
                out_buf.at[k, 4 * a : 4 * a + 4], outs[a].at[:, :, at], out_sem.at[k, a]
            )
            copy.start()
            stores.append(copy)
    for copy in stores:
        copy.wait()


def decode(slab, pieces):
    anywhere = pl.BlockSpec(memory_space=pl.ANY)
    vmem = pl.BlockSpec(memory_space=pltpu.VMEM)
    bf16 = jnp.bfloat16
    return pl.pallas_call(
        decode_kernel,
        in_specs=[vmem] + [anywhere] * 16,
        out_specs=[anywhere] * 3 + [vmem],
        out_shape=[jax.ShapeDtypeStruct((4, 64, 2048), bf16)] * 3
        + [jax.ShapeDtypeStruct((6, 128), jnp.float32)],
        scratch_shapes=[
            pltpu.VMEM((16, 768, 128), bf16),
            pltpu.VMEM((16, 12, 64, 128), bf16),
            pltpu.VMEM((128, 128), jnp.float32),
            pltpu.SemaphoreType.DMA((16,)),
            pltpu.SemaphoreType.DMA((16, 3)),
        ],
        cost_estimate=pl.CostEstimate(
            flops=20_000_000, bytes_accessed=6_300_000, transcendentals=3_000_000
        ),
        name="decode",
    )(slab, *pieces)


def on_device(w_gate, avg_gate, w_up, avg_up, w_down, avg_down, router_weight, router_gain):
    *pieces, slab = encode(
        (w_gate, avg_gate, w_up, avg_up, w_down, avg_down),
        router_weight.T,
        router_gain[None, :],
    )
    arrived = []
    for dz, dc in PARTNERS:
        pairs = [
            (2 * z + c, 2 * ((z + dz) % CHIPS) + (c ^ dc))
            for z in range(CHIPS)
            for c in range(2)
        ]
        arrived.append(lax.ppermute(pieces[2 * dz + dc], "fsdp", pairs))
    slab = lax.all_to_all(slab, "fsdp", 0, 0, tiled=True)
    router = slab[:, 12:16, :].transpose(1, 0, 2).reshape(4, 2048)
    router = lax.all_to_all(
        jnp.broadcast_to(router[None], (16, 4, 2048)), "ep", 0, 0, tiled=True
    )
    serve_router = router.reshape(64, 2048).T
    gate, up, down, scale = decode(slab, [pieces[0], *arrived])
    scale = jnp.concatenate([scale[:, :64], scale[:, 64:]], axis=0)
    return (
        gate.transpose(0, 2, 1),
        up.transpose(0, 2, 1),
        down,
        scale[0:4],
        scale[4:8],
        scale[8:12],
        serve_router,
    )


def solution(mesh):
    wide, tall = P("ep", "fsdp", None), P("ep", None, "fsdp")
    return jax.shard_map(
        on_device,
        mesh=mesh,
        in_specs=(wide, wide, wide, wide, tall, tall, P("fsdp", "ep"), P("fsdp")),
        out_specs=(tall, tall, wide, P("ep", "fsdp"), P("ep", "fsdp"), P("ep", "fsdp"), P()),
        check_vma=False,
    )
```

```python
import jax
import jax.numpy as jnp
from jax import lax
from jax.experimental import pallas as pl
from jax.experimental.pallas import tpu as pltpu
from jax.sharding import PartitionSpec as P


CHIPS = 8
POWER = 17.0
LIFT = 2.0 ** (126.0 / 17.0)
TINY = 1e-37
F32, BF16 = jnp.float32, jnp.bfloat16

PARTNERS = (
    (3, 0), (5, 0), (3, 1), (5, 1), (4, 0), (4, 1), (2, 0), (6, 0),
    (2, 1), (6, 1), (0, 1), (1, 0), (7, 0), (1, 1), (7, 1),
)
FIRST = (3, 5)
REST = (4, 2, 6, 0, 1, 7)
LATE = 4
AHEAD = 3


def position():
    me = lax.axis_index("fsdp")
    return lax.shift_right_logical(me, 1), lax.bitwise_and(me, 1)


def power(x):
    x2 = x * x
    x4 = x2 * x2
    x8 = x4 * x4
    return x8 * x8 * x


def encode_kernel(offsets, has_first, *refs):
    wg, ag, wu, au, wd, ad, router, gain = refs[:8]
    refs = refs[8:]
    if has_first:
        first, refs = refs[0], refs[1:]
    pieces, refs = refs[: 2 * len(offsets)], refs[2 * len(offsets) :]
    slab_ref, *bufs, out_buf, rows, sem, out_sem = refs
    chip, core = position()

    def target(g):
        return lax.rem(chip + g, CHIPS)

    def fetch(i):
        at = pl.ds(pl.multiple_of(target(offsets[i]) * 128, 128), 128)
        views = [r.at[:, :, at] for r in (wg, ag, wu, au)]
        views += [r.at[:, at, :] for r in (wd, ad)]
        return [
            pltpu.make_async_copy(v, b.at[i], sem.at[i, n])
            for n, (v, b) in enumerate(zip(views, bufs))
        ]

    copies = [fetch(i) for i in range(len(offsets))]
    for group in copies[:AHEAD]:
        for c in group:
            c.start()
    lane = lax.broadcasted_iota(jnp.int32, (128, 128), 1)
    left = lax.broadcasted_iota(jnp.int32, (6, 128), 1) < 64
    rows[12:16, :] = router[...] * gain[...]
    if has_first:
        for i, g in enumerate(FIRST):
            for c in range(2):
                slab_ref[target(g) * 2 + c] = first[2 * i + c]

    stores = []
    for i, g in enumerate(offsets):
        for c in copies[i]:
            c.wait()
        if i + AHEAD < len(offsets):
            for c in copies[i + AHEAD]:
                c.start()

        def put(q, y):
            at = slice(q * 64, q * 64 + 64)
            out_buf[2 * i, at, :] = y[:64]
            out_buf[2 * i + 1, at, :] = y[64:]

        sums = []
        for a in range(2):
            for e in range(4):
                fresh = bufs[2 * a][i, e] + bufs[2 * a + 1][i, e].astype(F32)
                total = jnp.sum(fresh * fresh, axis=0, keepdims=True)
                sums.append(total)
                y = power(fresh * (lax.rsqrt(jnp.maximum(total, TINY)) * LIFT))
                put(a * 4 + e, y.astype(BF16).T)
        tall = jnp.zeros((128, 128), F32)
        for e in range(4):
            fresh = bufs[4][i, e] + bufs[5][i, e].astype(F32)
            total = jnp.sum(fresh * fresh, axis=1, keepdims=True)
            tall = jnp.where(lane == e, total, tall)
            y = power(fresh * (lax.rsqrt(jnp.maximum(total, TINY)) * LIFT))
            put(8 + e, y.astype(BF16))
        for flip in range(2):
            copy = pltpu.make_async_copy(
                out_buf.at[2 * i + lax.bitwise_xor(core, flip)],
                pieces[2 * i + flip],
                out_sem.at[2 * i + flip],
            )
            copy.start()
            stores.append(copy)
        wide = tall.T
        top = jnp.concatenate(sums[:6], axis=0)
        bottom = jnp.concatenate(sums[6:] + [wide[0:4]], axis=0)
        both = (
            jnp.where(left, top, pltpu.roll(bottom, 64, 1)),
            jnp.where(left, pltpu.roll(top, 64, 1), bottom),
        )
        for c, s in enumerate(both):
            high = s.astype(BF16).astype(F32)
            rows[0:6, :] = high
            rows[6:12, :] = s - high
            at = target(g) * 2 + c if has_first else 2 * i + c
            slab_ref[at] = rows[...].astype(BF16)
    for copy in stores:
        copy.wait()


def encode(arrays, router, gain, offsets, first=None):
    n = len(offsets)
    anywhere = pl.BlockSpec(memory_space=pl.ANY)
    vmem = pl.BlockSpec(memory_space=pltpu.VMEM)
    given = [] if first is None else [first]
    slabs = 2 * n if first is None else 16

    def kernel(*refs):
        encode_kernel(offsets, first is not None, *refs)

    return pl.pallas_call(
        kernel,
        in_specs=[anywhere] * 6 + [vmem] * (2 + len(given)),
        out_specs=[anywhere] * (2 * n) + [vmem],
        out_shape=[jax.ShapeDtypeStruct((768, 128), BF16)] * (2 * n)
        + [jax.ShapeDtypeStruct((slabs, 16, 128), BF16)],
        scratch_shapes=[pltpu.VMEM((n, 4, 128, 128), t) for t in (F32, BF16) * 3]
        + [
            pltpu.VMEM((2 * n, 768, 128), BF16),
            pltpu.VMEM((16, 128), F32),
            pltpu.SemaphoreType.DMA((n, 6)),
            pltpu.SemaphoreType.DMA((2 * n,)),
        ],
        cost_estimate=pl.CostEstimate(
            flops=2_500_000 * n, bytes_accessed=1_600_000 * n, transcendentals=0
        ),
        name="encode_first" if first is None else "encode_rest",
    )(*arrays, router, gain, *given)


def norms_kernel(slab, gate_ref, up_ref, down_ref, table_ref, factors):
    chip, core = position()
    local, total = [], jnp.zeros((6, 128), F32)
    for dz, dc in ((0, 0), *PARTNERS):
        source = lax.rem(chip + CHIPS - dz, CHIPS) * 2 + lax.bitwise_xor(core, dc)
        both = slab[source].astype(F32)
        s = both[0:6] + both[6:12]
        local.append(s)
        total = total + s
    scale = jnp.sqrt(total)
    other = pltpu.roll(scale, 64, 1)
    gate_ref[...] = scale[0:4, :64]
    up_ref[0:2, :] = scale[4:6, :64]
    up_ref[2:4, :] = other[0:2, :64]
    down_ref[...] = other[2:6, :64]
    for k in range(16):
        factors[k * 8 : k * 8 + 6, :] = jnp.sqrt(local[k] / total) * (1.0 / LIFT)
        factors[k * 8 + 6 : k * 8 + 8, :] = jnp.zeros((2, 128), F32)
    table_ref[...] = factors[...].T


def norms(slab):
    vmem = pl.BlockSpec(memory_space=pltpu.VMEM)
    return pl.pallas_call(
        norms_kernel,
        in_specs=[vmem],
        out_specs=[vmem] * 4,
        out_shape=[jax.ShapeDtypeStruct((4, 64), F32)] * 3
        + [jax.ShapeDtypeStruct((128, 128), F32)],
        scratch_shapes=[pltpu.VMEM((128, 128), F32)],
        compiler_params=pltpu.CompilerParams(vmem_limit_bytes=2 << 20),
        cost_estimate=pl.CostEstimate(
            flops=1_000_000, bytes_accessed=200_000, transcendentals=0
        ),
        name="norms",
    )(slab)


def decode_kernel(which, has_outs, table, *refs):
    n = len(which)
    pieces, refs = refs[:n], refs[n:]
    if has_outs:
        refs = refs[3:]
    outs, (out_buf, sem) = refs[:3], refs[3:]
    chip, core = position()
    partners = ((0, 0), *PARTNERS)
    stores = []
    for i, k in enumerate(which):
        dz, dc = partners[k]
        source = lax.rem(chip + CHIPS - dz, CHIPS) * 2 + lax.bitwise_xor(core, dc)
        for q in range(12):
            half, lane = q // 6, k * 8 + q % 6
            factor = table[half * 64 : half * 64 + 64, lane : lane + 1]
            y = pieces[i][q * 64 : q * 64 + 64, :].astype(F32)
            x = jnp.exp2(jnp.log2(jnp.abs(y)) * (1.0 / POWER)) * factor
            out_buf[i, q] = jnp.where(y < 0, -x, x).astype(BF16)
            if q % 4 == 3:
                a = q // 4
                at = pl.ds(pl.multiple_of(source * 128, 128), 128)
                copy = pltpu.make_async_copy(
                    out_buf.at[i, 4 * a : 4 * a + 4],
                    outs[a].at[:, :, at],
                    sem.at[i, a],
                )
                copy.start()
                stores.append(copy)
    for copy in stores:
        copy.wait()


def decode(table, pieces, which, outs=()):
    n = len(which)
    anywhere = pl.BlockSpec(memory_space=pl.ANY)
    vmem = pl.BlockSpec(memory_space=pltpu.VMEM)

    def kernel(*refs):
        decode_kernel(which, bool(outs), *refs)

    return pl.pallas_call(
        kernel,
        in_specs=[vmem] * (1 + n) + [anywhere] * len(outs),
        out_specs=[anywhere] * 3,
        out_shape=[jax.ShapeDtypeStruct((4, 64, 2048), BF16)] * 3,
        input_output_aliases={1 + n + a: a for a in range(len(outs))},
        scratch_shapes=[
            pltpu.VMEM((n, 12, 64, 128), BF16),
            pltpu.SemaphoreType.DMA((n, 3)),
        ],
        compiler_params=pltpu.CompilerParams(vmem_limit_bytes=8 << 20),
        cost_estimate=pl.CostEstimate(
            flops=1_200_000 * n, bytes_accessed=400_000 * n, transcendentals=200_000 * n
        ),
        name="decode_late" if outs else "decode_early",
    )(table, *pieces, *outs)


def on_device(w_gate, avg_gate, w_up, avg_up, w_down, avg_down, router_weight, router_gain):
    arrays = (w_gate, avg_gate, w_up, avg_up, w_down, avg_down)
    router, gain = router_weight.T, router_gain[None, :]
    *some, slab = encode(arrays, router, gain, FIRST)
    *more, slab = encode(arrays, router, gain, REST, slab)
    pieces = dict(zip([(g, f) for g in FIRST + REST for f in range(2)], some + more))
    slab = lax.all_to_all(slab, "fsdp", 0, 0, tiled=True)
    arrived = [pieces[0, 0]]
    for dz, dc in PARTNERS:
        pairs = [
            (2 * z + c, 2 * ((z + dz) % CHIPS) + (c ^ dc))
            for z in range(CHIPS)
            for c in range(2)
        ]
        arrived.append(lax.ppermute(pieces[dz, dc], "fsdp", pairs))
    gate_scale, up_scale, down_scale, table = norms(slab)
    router = slab[:, 12:16, :].transpose(1, 0, 2).reshape(4, 2048)
    router = jnp.broadcast_to(router[None], (16, 4, 2048))
    router = lax.all_to_all(router, "ep", 0, 0, tiled=True)
    serve_router = router.reshape(64, 2048)
    early, late = tuple(range(16 - LATE)), tuple(range(16 - LATE, 16))
    outs = decode(table, [arrived[k] for k in early], early)
    table, serve_router = lax.optimization_barrier((table, serve_router))
    gate, up, down = decode(table, [arrived[k] for k in late], late, tuple(outs))
    return (
        gate.transpose(0, 2, 1),
        up.transpose(0, 2, 1),
        down,
        gate_scale,
        up_scale,
        down_scale,
        serve_router.T,
    )


def solution(mesh):
    wide, tall = P("ep", "fsdp", None), P("ep", None, "fsdp")

    return jax.shard_map(
        on_device,
        mesh=mesh,
        in_specs=(wide, wide, wide, wide, tall, tall, P("fsdp", "ep"), P("fsdp")),
        out_specs=(tall, tall, wide, P("ep", "fsdp"), P("ep", "fsdp"), P("ep", "fsdp"), P()),
        check_vma=False,
    )
```

```python
import jax
import jax.numpy as jnp
from jax import lax
from jax.experimental import pallas as pl
from jax.experimental.pallas import tpu as pltpu
from jax.sharding import PartitionSpec as P


CHIPS = 8
POWER = 17.0
LIFT = 2.0 ** (126.0 / 17.0)
TINY = 1e-37
F32, BF16 = jnp.float32, jnp.bfloat16

PARTNERS = (
    (4, 0), (4, 1), (3, 0), (5, 0), (1, 0), (7, 0), (1, 1), (7, 1),
    (2, 0), (6, 0), (0, 1), (2, 1), (6, 1), (3, 1), (5, 1),
)
FIRST = 4
REST = (3, 5, 2, 6, 0, 1, 7)
STAGES = (12, 14, 16)
AHEAD = 8


def position():
    me = lax.axis_index("fsdp")
    return lax.shift_right_logical(me, 1), lax.bitwise_and(me, 1)


def power(x):
    x2 = x * x
    x4 = x2 * x2
    x8 = x4 * x4
    return x8 * x8 * x


def normalised(fresh, axis):
    total = jnp.sum(fresh * fresh, axis=axis, keepdims=True)
    y = power(fresh * (lax.rsqrt(jnp.maximum(total, TINY)) * LIFT))
    return total, y.astype(BF16)


def send_off(out_buf, pieces, sem, i, part, parts, stores):
    _, core = position()
    size = 768 // parts
    at = pl.ds(part * size, size)
    for flip in range(2):
        copy = pltpu.make_async_copy(
            out_buf.at[2 * i + lax.bitwise_xor(core, flip), at],
            pieces[2 * i + flip].at[at],
            sem.at[2 * i + flip, part],
        )
        copy.start()
        stores.append(copy)


def first_kernel(wg, ag, wu, au, wd, ad, piece_0, piece_1, sums_out, *scratch):
    *bufs, out_buf, sums, sem, out_sem, sums_sem = scratch
    chip, _ = position()
    at = pl.ds(pl.multiple_of(lax.rem(chip + FIRST, CHIPS) * 128, 128), 128)
    views = [r.at[:, :, at] for r in (wg, ag, wu, au)]
    views += [r.at[:, at, :] for r in (wd, ad)]
    copies = [
        pltpu.make_async_copy(v, b, sem.at[n]) for n, (v, b) in enumerate(zip(views, bufs))
    ]
    for c in copies:
        c.start()
    lane = lax.broadcasted_iota(jnp.int32, (128, 128), 1)
    tall = jnp.zeros((128, 128), F32)
    stores = []
    for a in range(3):
        copies[2 * a].wait()
        copies[2 * a + 1].wait()
        for e in range(4):
            q = a * 4 + e
            fresh = bufs[2 * a][e] + bufs[2 * a + 1][e].astype(F32)
            total, y = normalised(fresh, 0 if a < 2 else 1)
            if a < 2:
                sums[q : q + 1, :] = total
                y = y.T
            else:
                tall = jnp.where(lane == e, total, tall)
            out_buf[0, q * 64 : q * 64 + 64, :] = y[:64]
            out_buf[1, q * 64 : q * 64 + 64, :] = y[64:]
        send_off(out_buf, (piece_0, piece_1), out_sem, 0, a, 3, stores)
    sums[8:16, :] = tall.T[0:8]
    copy = pltpu.make_async_copy(sums, sums_out, sums_sem)
    copy.start()
    for c in (*stores, copy):
        c.wait()


def encode_first(arrays):
    anywhere = pl.BlockSpec(memory_space=pl.ANY)
    return pl.pallas_call(
        first_kernel,
        in_specs=[anywhere] * 6,
        out_specs=[anywhere] * 3,
        out_shape=[jax.ShapeDtypeStruct((768, 128), BF16)] * 2
        + [jax.ShapeDtypeStruct((16, 128), F32)],
        scratch_shapes=[pltpu.VMEM((4, 128, 128), t) for t in (F32, BF16) * 3]
        + [
            pltpu.VMEM((2, 768, 128), BF16),
            pltpu.VMEM((16, 128), F32),
            pltpu.SemaphoreType.DMA((6,)),
            pltpu.SemaphoreType.DMA((2, 3)),
            pltpu.SemaphoreType.DMA,
        ],
        cost_estimate=pl.CostEstimate(
            flops=2_500_000, bytes_accessed=1_600_000, transcendentals=0
        ),
        name="encode_first",
    )(*arrays)


def rest_kernel(wg, ag, wu, au, wd, ad, router, gain, first_sums, *refs):
    n = len(REST)
    pieces, slab_out = refs[: 2 * n], refs[2 * n]
    *bufs, out_buf, tall, sums, rows, slab_buf, router_buf, gain_buf = refs[2 * n + 1 : -3]
    sem, out_sem, small_sem = refs[-3:]
    chip, _ = position()

    def target(g):
        return lax.rem(chip + g, CHIPS)

    arrays = (wg, ag, wu, au, wd, ad)
    copies = [
        [
            pltpu.make_async_copy(arrays[m].at[e], bufs[m].at[e], sem.at[m, e])
            for m in (2 * a, 2 * a + 1)
        ]
        for a in range(3)
        for e in range(4)
    ]
    small = [
        pltpu.make_async_copy(router, router_buf, small_sem.at[0]),
        pltpu.make_async_copy(gain, gain_buf, small_sem.at[1]),
        pltpu.make_async_copy(first_sums, sums.at[n], small_sem.at[2]),
    ]
    for some in copies[:AHEAD]:
        for c in some:
            c.start()
    for c in small:
        c.start()
    lane = lax.broadcasted_iota(jnp.int32, (128, 128), 1)
    left = lax.broadcasted_iota(jnp.int32, (6, 128), 1) < 64

    stores = []
    for q in range(12):
        a, e = q // 4, q % 4
        for c in copies[q]:
            c.wait()
        if q + AHEAD < 12:
            for c in copies[q + AHEAD]:
                c.start()
        for i, g in enumerate(REST):
            at = pl.ds(pl.multiple_of(target(g) * 128, 128), 128)
            where = (e, slice(None), at) if a < 2 else (e, at, slice(None))
            fresh = bufs[2 * a][where] + bufs[2 * a + 1][where].astype(F32)
            total, y = normalised(fresh, 0 if a < 2 else 1)
            if a < 2:
                sums[i, q : q + 1, :] = total
                y = y.T
            elif e == 0:
                tall[i] = jnp.where(lane == 0, total, 0.0)
            else:
                tall[i] = jnp.where(lane == e, total, tall[i])
            out_buf[2 * i, q * 64 : q * 64 + 64, :] = y[:64]
            out_buf[2 * i + 1, q * 64 : q * 64 + 64, :] = y[64:]
        if q % 2 == 1:
            for i in range(n):
                send_off(out_buf, pieces, out_sem, i, q // 2, 6, stores)
    for c in small:
        c.wait()
    rows[12:16, :] = router_buf[...] * gain_buf[...]
    for i, g in enumerate((*REST, FIRST)):
        if i < n:
            sums[i, 8:16, :] = tall[i].T[0:8]
        top, bottom = sums[i, 0:6, :], sums[i, 6:12, :]
        both = (
            jnp.where(left, top, pltpu.roll(bottom, 64, 1)),
            jnp.where(left, pltpu.roll(top, 64, 1), bottom),
        )
        for c, s in enumerate(both):
            high = s.astype(BF16).astype(F32)
            rows[0:6, :] = high
            rows[6:12, :] = s - high
            slab_buf[target(g) * 2 + c] = rows[...].astype(BF16)
    copy = pltpu.make_async_copy(slab_buf, slab_out, small_sem.at[3])
    copy.start()
    for c in (*stores, copy):
        c.wait()


def encode_rest(arrays, router, gain, first_sums):
    n = len(REST)
    anywhere = pl.BlockSpec(memory_space=pl.ANY)
    return pl.pallas_call(
        rest_kernel,
        in_specs=[anywhere] * 9,
        out_specs=[anywhere] * (2 * n + 1),
        out_shape=[jax.ShapeDtypeStruct((768, 128), BF16)] * (2 * n)
        + [jax.ShapeDtypeStruct((16, 16, 128), BF16)],
        scratch_shapes=[
            pltpu.VMEM(shape, t)
            for shape in ((4, 128, 1024), (4, 128, 1024), (4, 1024, 128))
            for t in (F32, BF16)
        ]
        + [
            pltpu.VMEM((2 * n, 768, 128), BF16),
            pltpu.VMEM((n, 128, 128), F32),
            pltpu.VMEM((n + 1, 16, 128), F32),
            pltpu.VMEM((16, 128), F32),
            pltpu.VMEM((16, 16, 128), BF16),
            pltpu.VMEM((4, 128), F32),
            pltpu.VMEM((1, 128), F32),
            pltpu.SemaphoreType.DMA((6, 4)),
            pltpu.SemaphoreType.DMA((2 * n, 6)),
            pltpu.SemaphoreType.DMA((4,)),
        ],
        cost_estimate=pl.CostEstimate(
            flops=2_500_000 * n, bytes_accessed=1_600_000 * n, transcendentals=0
        ),
        name="encode_rest",
    )(*arrays, router, gain, first_sums)


def norms_kernel(slab, gate_ref, up_ref, down_ref, table_ref, factors):
    chip, core = position()
    local, total = [], jnp.zeros((6, 128), F32)
    for dz, dc in ((0, 0), *PARTNERS):
        source = lax.rem(chip + CHIPS - dz, CHIPS) * 2 + lax.bitwise_xor(core, dc)
        both = slab[source].astype(F32)
        s = both[0:6] + both[6:12]
        local.append(s)
        total = total + s
    scale = jnp.sqrt(total)
    other = pltpu.roll(scale, 64, 1)
    gate_ref[...] = scale[0:4, :64]
    up_ref[0:2, :] = scale[4:6, :64]
    up_ref[2:4, :] = other[0:2, :64]
    down_ref[...] = other[2:6, :64]
    for k in range(16):
        factors[k * 8 : k * 8 + 6, :] = jnp.sqrt(local[k] / total) * (1.0 / LIFT)
        factors[k * 8 + 6 : k * 8 + 8, :] = jnp.zeros((2, 128), F32)
    table_ref[...] = factors[...].T


def norms(slab):
    vmem = pl.BlockSpec(memory_space=pltpu.VMEM)
    return pl.pallas_call(
        norms_kernel,
        in_specs=[vmem],
        out_specs=[vmem] * 4,
        out_shape=[jax.ShapeDtypeStruct((4, 64), F32)] * 3
        + [jax.ShapeDtypeStruct((128, 128), F32)],
        scratch_shapes=[pltpu.VMEM((128, 128), F32)],
        compiler_params=pltpu.CompilerParams(vmem_limit_bytes=2 << 20),
        cost_estimate=pl.CostEstimate(
            flops=1_000_000, bytes_accessed=200_000, transcendentals=0
        ),
        name="norms",
    )(slab)


def decode_kernel(which, has_outs, table, *refs):
    n = len(which)
    pieces, refs = refs[:n], refs[n:]
    if has_outs:
        refs = refs[3:]
    outs, (out_buf, sem) = refs[:3], refs[3:]
    chip, core = position()
    partners = ((0, 0), *PARTNERS)
    stores = []
    for i, k in enumerate(which):
        dz, dc = partners[k]
        source = lax.rem(chip + CHIPS - dz, CHIPS) * 2 + lax.bitwise_xor(core, dc)
        for q in range(12):
            half, lane = q // 6, k * 8 + q % 6
            factor = table[half * 64 : half * 64 + 64, lane : lane + 1]
            y = pieces[i][q * 64 : q * 64 + 64, :].astype(F32)
            x = jnp.exp2(jnp.log2(jnp.abs(y)) * (1.0 / POWER)) * factor
            out_buf[i, q] = jnp.where(y < 0, -x, x).astype(BF16)
            if q % 4 == 3:
                a = q // 4
                at = pl.ds(pl.multiple_of(source * 128, 128), 128)
                copy = pltpu.make_async_copy(
                    out_buf.at[i, 4 * a : 4 * a + 4],
                    outs[a].at[:, :, at],
                    sem.at[i, a],
                )
                copy.start()
                stores.append(copy)
    for copy in stores:
        copy.wait()


def decode(table, pieces, which, outs):
    n = len(which)
    anywhere = pl.BlockSpec(memory_space=pl.ANY)
    vmem = pl.BlockSpec(memory_space=pltpu.VMEM)

    def kernel(*refs):
        decode_kernel(which, bool(outs), *refs)

    return pl.pallas_call(
        kernel,
        in_specs=[vmem] * (1 + n) + [anywhere] * len(outs),
        out_specs=[anywhere] * 3,
        out_shape=[jax.ShapeDtypeStruct((4, 64, 2048), BF16)] * 3,
        input_output_aliases={1 + n + a: a for a in range(len(outs))},
        scratch_shapes=[
            pltpu.VMEM((n, 12, 64, 128), BF16),
            pltpu.SemaphoreType.DMA((n, 3)),
        ],
        compiler_params=pltpu.CompilerParams(vmem_limit_bytes=8 << 20),
        cost_estimate=pl.CostEstimate(
            flops=1_200_000 * n, bytes_accessed=400_000 * n, transcendentals=200_000 * n
        ),
    )(table, *pieces, *outs)


def on_device(w_gate, avg_gate, w_up, avg_up, w_down, avg_down, router_weight, router_gain):
    arrays = (w_gate, avg_gate, w_up, avg_up, w_down, avg_down)
    router, gain = router_weight.T, router_gain[None, :]
    *some, first_sums = encode_first(arrays)
    *more, slab = encode_rest(arrays, router, gain, first_sums)
    pieces = dict(zip([(g, f) for g in (FIRST, *REST) for f in range(2)], some + more))
    slab = lax.all_to_all(slab, "fsdp", 0, 0, tiled=True)
    arrived = [pieces[0, 0]]
    for dz, dc in PARTNERS:
        pairs = [
            (2 * z + c, 2 * ((z + dz) % CHIPS) + (c ^ dc))
            for z in range(CHIPS)
            for c in range(2)
        ]
        arrived.append(lax.ppermute(pieces[dz, dc], "fsdp", pairs))
    gate_scale, up_scale, down_scale, table = norms(slab)
    router = slab[:, 12:16, :].transpose(1, 0, 2).reshape(4, 2048)
    router = jnp.broadcast_to(router[None], (16, 4, 2048))
    router = lax.all_to_all(router, "ep", 0, 0, tiled=True)
    serve_router = router.reshape(64, 2048)
    outs, done = (), 0
    for stage, end in enumerate(STAGES):
        which = tuple(range(done, end))
        outs = decode(table, [arrived[k] for k in which], which, tuple(outs))
        if stage == 0:
            table, serve_router = lax.optimization_barrier((table, serve_router))
        done = end
    gate, up, down = outs
    return (
        gate.transpose(0, 2, 1),
        up.transpose(0, 2, 1),
        down,
        gate_scale,
        up_scale,
        down_scale,
        serve_router.T,
    )


def solution(mesh):
    wide, tall = P("ep", "fsdp", None), P("ep", None, "fsdp")

    return jax.shard_map(
        on_device,
        mesh=mesh,
        in_specs=(wide, wide, wide, wide, tall, tall, P("fsdp", "ep"), P("fsdp")),
        out_specs=(tall, tall, wide, P("ep", "fsdp"), P("ep", "fsdp"), P("ep", "fsdp"), P()),
        check_vma=False,
    )
```

```python
import jax
import jax.numpy as jnp
from jax import lax
from jax.experimental import pallas as pl
from jax.experimental.pallas import tpu as pltpu
from jax.sharding import PartitionSpec as P


CHIPS = 8
POWER = 17.0
LIFT = 2.0 ** (126.0 / 17.0)
TINY = 1e-37
F32, BF16 = jnp.float32, jnp.bfloat16

PARTNERS = (
    (3, 0), (3, 1), (4, 0), (4, 1), (2, 0), (6, 0), (1, 0), (7, 0),
    (2, 1), (6, 1), (1, 1), (7, 1), (0, 1), (5, 0), (5, 1),
)
FIRST = 3
REST = (4, 5, 2, 6, 0, 1, 7)
STAGES = (12, 14, 16)
AHEAD = 8


def position():
    me = lax.axis_index("fsdp")
    return lax.shift_right_logical(me, 1), lax.bitwise_and(me, 1)


def away(chip, core, g):
    return lax.rem(chip + jnp.where(core == 0, g, CHIPS - g), CHIPS)


def source_of(chip, core, partner):
    dz, dc = partner
    sender = lax.bitwise_xor(core, dc)
    return away(chip, 1 - sender, dz) * 2 + sender


def power(x):
    x2 = x * x
    x4 = x2 * x2
    x8 = x4 * x4
    return x8 * x8 * x


def normalised(fresh, axis):
    total = jnp.sum(fresh * fresh, axis=axis, keepdims=True)
    y = power(fresh * (lax.rsqrt(jnp.maximum(total, TINY)) * LIFT))
    return total, y.astype(BF16)


def send_off(out_buf, pieces, sem, i, part, parts, stores):
    _, core = position()
    size = 768 // parts
    at = pl.ds(part * size, size)
    for flip in range(2):
        copy = pltpu.make_async_copy(
            out_buf.at[2 * i + lax.bitwise_xor(core, flip), at],
            pieces[2 * i + flip].at[at],
            sem.at[2 * i + flip, part],
        )
        copy.start()
        stores.append(copy)


def first_kernel(wg, ag, wu, au, wd, ad, piece_0, piece_1, sums_out, *scratch):
    *bufs, out_buf, sums, sem, out_sem, sums_sem = scratch
    chip, core = position()
    at = pl.ds(pl.multiple_of(away(chip, core, FIRST) * 128, 128), 128)
    views = [r.at[:, :, at] for r in (wg, ag, wu, au)]
    views += [r.at[:, at, :] for r in (wd, ad)]
    copies = [
        pltpu.make_async_copy(v, b, sem.at[n]) for n, (v, b) in enumerate(zip(views, bufs))
    ]
    for c in copies:
        c.start()
    lane = lax.broadcasted_iota(jnp.int32, (128, 128), 1)
    tall = jnp.zeros((128, 128), F32)
    stores = []
    for a in range(3):
        copies[2 * a].wait()
        copies[2 * a + 1].wait()
        for e in range(4):
            q = a * 4 + e
            fresh = bufs[2 * a][e] + bufs[2 * a + 1][e].astype(F32)
            total, y = normalised(fresh, 0 if a < 2 else 1)
            if a < 2:
                sums[q : q + 1, :] = total
                y = y.T
            else:
                tall = jnp.where(lane == e, total, tall)
            out_buf[0, q * 64 : q * 64 + 64, :] = y[:64]
            out_buf[1, q * 64 : q * 64 + 64, :] = y[64:]
        send_off(out_buf, (piece_0, piece_1), out_sem, 0, a, 3, stores)
    sums[8:16, :] = tall.T[0:8]
    copy = pltpu.make_async_copy(sums, sums_out, sums_sem)
    copy.start()
    for c in (*stores, copy):
        c.wait()


def encode_first(arrays):
    anywhere = pl.BlockSpec(memory_space=pl.ANY)
    return pl.pallas_call(
        first_kernel,
        in_specs=[anywhere] * 6,
        out_specs=[anywhere] * 3,
        out_shape=[jax.ShapeDtypeStruct((768, 128), BF16)] * 2
        + [jax.ShapeDtypeStruct((16, 128), F32)],
        scratch_shapes=[pltpu.VMEM((4, 128, 128), t) for t in (F32, BF16) * 3]
        + [
            pltpu.VMEM((2, 768, 128), BF16),
            pltpu.VMEM((16, 128), F32),
            pltpu.SemaphoreType.DMA((6,)),
            pltpu.SemaphoreType.DMA((2, 3)),
            pltpu.SemaphoreType.DMA,
        ],
        cost_estimate=pl.CostEstimate(
            flops=2_500_000, bytes_accessed=1_600_000, transcendentals=0
        ),
        name="encode_first",
    )(*arrays)


def rest_kernel(wg, ag, wu, au, wd, ad, router, gain, first_sums, *refs):
    n = len(REST)
    pieces, slab_out = refs[: 2 * n], refs[2 * n]
    *bufs, out_buf, tall, sums, rows, slab_buf, router_buf, gain_buf = refs[2 * n + 1 : -3]
    sem, out_sem, small_sem = refs[-3:]
    chip, core = position()

    def target(g):
        return away(chip, core, g)

    arrays = (wg, ag, wu, au, wd, ad)
    copies = [
        [
            pltpu.make_async_copy(arrays[m].at[e], bufs[m].at[e], sem.at[m, e])
            for m in (2 * a, 2 * a + 1)
        ]
        for a in range(3)
        for e in range(4)
    ]
    small = [
        pltpu.make_async_copy(router, router_buf, small_sem.at[0]),
        pltpu.make_async_copy(gain, gain_buf, small_sem.at[1]),
        pltpu.make_async_copy(first_sums, sums.at[n], small_sem.at[2]),
    ]
    for some in copies[:AHEAD]:
        for c in some:
            c.start()
    for c in small:
        c.start()
    lane = lax.broadcasted_iota(jnp.int32, (128, 128), 1)
    left = lax.broadcasted_iota(jnp.int32, (6, 128), 1) < 64

    stores = []
    for q in range(12):
        a, e = q // 4, q % 4
        for c in copies[q]:
            c.wait()
        if q + AHEAD < 12:
            for c in copies[q + AHEAD]:
                c.start()
        for i, g in enumerate(REST):
            at = pl.ds(pl.multiple_of(target(g) * 128, 128), 128)
            where = (e, slice(None), at) if a < 2 else (e, at, slice(None))
            fresh = bufs[2 * a][where] + bufs[2 * a + 1][where].astype(F32)
            total, y = normalised(fresh, 0 if a < 2 else 1)
            if a < 2:
                sums[i, q : q + 1, :] = total
                y = y.T
            elif e == 0:
                tall[i] = jnp.where(lane == 0, total, 0.0)
            else:
                tall[i] = jnp.where(lane == e, total, tall[i])
            out_buf[2 * i, q * 64 : q * 64 + 64, :] = y[:64]
            out_buf[2 * i + 1, q * 64 : q * 64 + 64, :] = y[64:]
        if q % 2 == 1:
            for i in range(n):
                send_off(out_buf, pieces, out_sem, i, q // 2, 6, stores)
    for c in small:
        c.wait()
    rows[12:16, :] = router_buf[...] * gain_buf[...]
    for i, g in enumerate((*REST, FIRST)):
        if i < n:
            sums[i, 8:16, :] = tall[i].T[0:8]
        top, bottom = sums[i, 0:6, :], sums[i, 6:12, :]
        both = (
            jnp.where(left, top, pltpu.roll(bottom, 64, 1)),
            jnp.where(left, pltpu.roll(top, 64, 1), bottom),
        )
        for c, s in enumerate(both):
            high = s.astype(BF16).astype(F32)
            rows[0:6, :] = high
            rows[6:12, :] = s - high
            slab_buf[target(g) * 2 + c] = rows[...].astype(BF16)
    copy = pltpu.make_async_copy(slab_buf, slab_out, small_sem.at[3])
    copy.start()
    for c in (*stores, copy):
        c.wait()


def encode_rest(arrays, router, gain, first_sums):
    n = len(REST)
    anywhere = pl.BlockSpec(memory_space=pl.ANY)
    return pl.pallas_call(
        rest_kernel,
        in_specs=[anywhere] * 9,
        out_specs=[anywhere] * (2 * n + 1),
        out_shape=[jax.ShapeDtypeStruct((768, 128), BF16)] * (2 * n)
        + [jax.ShapeDtypeStruct((16, 16, 128), BF16)],
        scratch_shapes=[
            pltpu.VMEM(shape, t)
            for shape in ((4, 128, 1024), (4, 128, 1024), (4, 1024, 128))
            for t in (F32, BF16)
        ]
        + [
            pltpu.VMEM((2 * n, 768, 128), BF16),
            pltpu.VMEM((n, 128, 128), F32),
            pltpu.VMEM((n + 1, 16, 128), F32),
            pltpu.VMEM((16, 128), F32),
            pltpu.VMEM((16, 16, 128), BF16),
            pltpu.VMEM((4, 128), F32),
            pltpu.VMEM((1, 128), F32),
            pltpu.SemaphoreType.DMA((6, 4)),
            pltpu.SemaphoreType.DMA((2 * n, 6)),
            pltpu.SemaphoreType.DMA((4,)),
        ],
        cost_estimate=pl.CostEstimate(
            flops=2_500_000 * n, bytes_accessed=1_600_000 * n, transcendentals=0
        ),
        name="encode_rest",
    )(*arrays, router, gain, first_sums)


def norms_kernel(slab, gate_ref, up_ref, down_ref, table_ref, factors):
    chip, core = position()
    local, total = [], jnp.zeros((6, 128), F32)
    for partner in ((0, 0), *PARTNERS):
        both = slab[source_of(chip, core, partner)].astype(F32)
        s = both[0:6] + both[6:12]
        local.append(s)
        total = total + s
    scale = jnp.sqrt(total)
    other = pltpu.roll(scale, 64, 1)
    gate_ref[...] = scale[0:4, :64]
    up_ref[0:2, :] = scale[4:6, :64]
    up_ref[2:4, :] = other[0:2, :64]
    down_ref[...] = other[2:6, :64]
    for k in range(16):
        factors[k * 8 : k * 8 + 6, :] = jnp.sqrt(local[k] / total) * (1.0 / LIFT)
        factors[k * 8 + 6 : k * 8 + 8, :] = jnp.zeros((2, 128), F32)
    table_ref[...] = factors[...].T


def norms(slab):
    vmem = pl.BlockSpec(memory_space=pltpu.VMEM)
    return pl.pallas_call(
        norms_kernel,
        in_specs=[vmem],
        out_specs=[vmem] * 4,
        out_shape=[jax.ShapeDtypeStruct((4, 64), F32)] * 3
        + [jax.ShapeDtypeStruct((128, 128), F32)],
        scratch_shapes=[pltpu.VMEM((128, 128), F32)],
        compiler_params=pltpu.CompilerParams(vmem_limit_bytes=2 << 20),
        cost_estimate=pl.CostEstimate(
            flops=1_000_000, bytes_accessed=200_000, transcendentals=0
        ),
        name="norms",
    )(slab)


def decode_kernel(which, has_outs, table, *refs):
    n = len(which)
    pieces, refs = refs[:n], refs[n:]
    if has_outs:
        refs = refs[3:]
    outs, (out_buf, sem) = refs[:3], refs[3:]
    chip, core = position()
    partners = ((0, 0), *PARTNERS)
    stores = []
    for i, k in enumerate(which):
        source = source_of(chip, core, partners[k])
        for q in range(12):
            half, lane = q // 6, k * 8 + q % 6
            factor = table[half * 64 : half * 64 + 64, lane : lane + 1]
            y = pieces[i][q * 64 : q * 64 + 64, :].astype(F32)
            x = jnp.exp2(jnp.log2(jnp.abs(y)) * (1.0 / POWER)) * factor
            out_buf[i, q] = jnp.where(y < 0, -x, x).astype(BF16)
            if q % 4 == 3:
                a = q // 4
                at = pl.ds(pl.multiple_of(source * 128, 128), 128)
                copy = pltpu.make_async_copy(
                    out_buf.at[i, 4 * a : 4 * a + 4],
                    outs[a].at[:, :, at],
                    sem.at[i, a],
                )
                copy.start()
                stores.append(copy)
    for copy in stores:
        copy.wait()


def decode(table, pieces, which, outs):
    n = len(which)
    anywhere = pl.BlockSpec(memory_space=pl.ANY)
    vmem = pl.BlockSpec(memory_space=pltpu.VMEM)

    def kernel(*refs):
        decode_kernel(which, bool(outs), *refs)

    return pl.pallas_call(
        kernel,
        in_specs=[vmem] * (1 + n) + [anywhere] * len(outs),
        out_specs=[anywhere] * 3,
        out_shape=[jax.ShapeDtypeStruct((4, 64, 2048), BF16)] * 3,
        input_output_aliases={1 + n + a: a for a in range(len(outs))},
        scratch_shapes=[
            pltpu.VMEM((n, 12, 64, 128), BF16),
            pltpu.SemaphoreType.DMA((n, 3)),
        ],
        compiler_params=pltpu.CompilerParams(vmem_limit_bytes=8 << 20),
        cost_estimate=pl.CostEstimate(
            flops=1_200_000 * n, bytes_accessed=400_000 * n, transcendentals=200_000 * n
        ),
    )(table, *pieces, *outs)


def on_device(w_gate, avg_gate, w_up, avg_up, w_down, avg_down, router_weight, router_gain):
    arrays = (w_gate, avg_gate, w_up, avg_up, w_down, avg_down)
    router, gain = router_weight.T, router_gain[None, :]
    *some, first_sums = encode_first(arrays)
    *more, slab = encode_rest(arrays, router, gain, first_sums)
    pieces = dict(zip([(g, f) for g in (FIRST, *REST) for f in range(2)], some + more))
    slab = lax.all_to_all(slab, "fsdp", 0, 0, tiled=True)
    arrived = [pieces[0, 0]]
    for dz, dc in PARTNERS:
        pairs = [
            (2 * z + c, 2 * ((z + (dz, CHIPS - dz)[c]) % CHIPS) + (c ^ dc))
            for z in range(CHIPS)
            for c in range(2)
        ]
        arrived.append(lax.ppermute(pieces[dz, dc], "fsdp", pairs))
    gate_scale, up_scale, down_scale, table = norms(slab)
    router = slab[:, 12:16, :].transpose(1, 0, 2).reshape(4, 2048)
    router = jnp.broadcast_to(router[None], (16, 4, 2048))
    router = lax.all_to_all(router, "ep", 0, 0, tiled=True)
    serve_router = router.reshape(64, 2048)
    outs, done = (), 0
    for stage, end in enumerate(STAGES):
        which = tuple(range(done, end))
        outs = decode(table, [arrived[k] for k in which], which, tuple(outs))
        if stage == 0:
            table, serve_router = lax.optimization_barrier((table, serve_router))
        done = end
    gate, up, down = outs
    return (
        gate.transpose(0, 2, 1),
        up.transpose(0, 2, 1),
        down,
        gate_scale,
        up_scale,
        down_scale,
        serve_router.T,
    )


def solution(mesh):
    wide, tall = P("ep", "fsdp", None), P("ep", None, "fsdp")

    return jax.shard_map(
        on_device,
        mesh=mesh,
        in_specs=(wide, wide, wide, wide, tall, tall, P("fsdp", "ep"), P("fsdp")),
        out_specs=(tall, tall, wide, P("ep", "fsdp"), P("ep", "fsdp"), P("ep", "fsdp"), P()),
        check_vma=False,
    )
```
